256 devices in a mesh: section: 4 (over y), node: 8 (over z), torus: 8 (over x, core).
Axes of the slice: x: 4, y: 4, z: 8, core: 2. Of those that a mesh axis runs over, the one named last changes fastest.
Arguments:
- act_in: bfloat16 [4, 2048, 7168], P('section', 'node', 'torus'), may hold values from -28 to 28
- next_in: bfloat16 [2048, 7168], P('node', 'torus'), may hold values from -42 to 42
- routes: int32 [2, 4, 2048, 2], P(None, 'section', 'node'), may hold values from 0 to 7, all different within a row; in each aligned block of 256 rows (0 to 255, 256 to 511, ..., all dimensions but the last counted through in order) at most 80 rows name the same one
- route_w: float32 [2, 4, 2048, 2], P(None, 'section', 'node'), may hold values from 0.2 to 1
- hist: float32 [4], P('section'), may hold values from 2 to 8
- gate_w: bfloat16 [4, 8, 7168, 1024], P('section', 'node', 'torus'), may hold values from -0.0625 to 0.0625
- up_w: bfloat16 [4, 8, 7168, 1024], P('section', 'node', 'torus'), may hold values from -0.0625 to 0.0625
- down_w: bfloat16 [4, 8, 1024, 7168], P('section', 'node', None, 'torus'), may hold values from -0.09375 to 0.09375
Outputs:
- act_out: bfloat16 [2, 4, 2048, 7168], P(None, 'section', 'node', 'torus')
- peak_out: float32 [4, 2], P('section')
The draws below stay inside these ranges and needn't reach their ends.
Inputs may be any that keep to these rules, and one draw needn't show every extreme that they name: `routes`: each token names 2 different experts; within the 256 tokens of one index of node (aligned blocks of rows of one tick and layer) no expert is named more than 80 times, a bound that some block reaches.
All inputs are finite; a program needn't handle non-finite values.
Results may differ from the reference program's by a relative error of at most 0.012.
Values may be sent and summed in bfloat16 or wider, within the bound.
No kernel may reach another device: no remote copies, remote signals or barrier semaphores. Data moves between devices by JAX's collectives and lax.ppermute only.
A program may use at most 64 MiB of HBM per device.

```python
import math
import jax
import jax.numpy as jnp
import numpy as np
from jax import lax

D = 7168
FFW = 1024
TOPK = 2
TICKS = 2
TOK_DEV = 256
SECTIONS = 4
EXPERTS = 8
CAP = 80
TOKENS = 2048
N_NODE = 8


def rising_rows(key, array_shape, factor):
    noise_key, scale_key = jax.random.split(key)
    rising = 1.0 + 2.0 * jnp.arange(TOKENS, dtype=jnp.float32) / TOKENS
    noise = jnp.clip(jax.random.normal(noise_key, array_shape, jnp.float32), -6.0, 6.0)
    spread = jnp.exp(jax.random.uniform(scale_key, array_shape[:-1] + (1,), jnp.float32, -0.7, 0.4))
    return (noise * spread * rising[:, None] * factor).astype(jnp.bfloat16)


def draw_act_in(key, part):
    return rising_rows(jax.random.fold_in(key, 11), (SECTIONS, TOKENS, D), 1.0)


def draw_next_in(key, part):
    return rising_rows(jax.random.fold_in(key, 23), (TOKENS, D), 1.5)


def levels(stream_key, dims, shards, low, top_value):
    level, own = 1.0, jax.random.fold_in(stream_key, 6)
    for axis_at, blocks in shards:
        steps = jnp.exp(jax.random.uniform(jax.random.fold_in(own, axis_at), (blocks,), jnp.float32, low / len(shards), top_value / len(shards)))
        level = level * jnp.repeat(steps, dims[axis_at] // blocks).reshape([-1 if axis == axis_at else 1 for axis in range(len(dims))])
    return level


def routed_block(own_key, own, number, rows, amount, top, reach, lean):
    order = jax.random.permutation(own_key, amount)
    heavy_load, ordinary = shares(amount, rows * top, reach, lean, True), shares(amount, rows * top, reach, lean, False)
    places = jnp.arange(amount)

    def named(tallies, turn):
        used = int((tallies > 0).sum())
        fixed = max(1, used // 4)
        shifted = fixed + (places - fixed + turn * (used - fixed)) % max(1, amount - fixed)
        return jnp.zeros((amount,), jnp.int32).at[order[jnp.where(places < fixed, places, shifted)]].set(jnp.asarray(tallies, jnp.int32))

    tallies = jnp.where(number % 4 == 0, named(heavy_load, number // 4), named(ordinary, number - number // 4 - 1))
    mixed = jax.random.permutation(jax.random.fold_in(own, 3), amount)
    source_of, sink = mixed[0:amount // 2 * 2:2], mixed[1:amount // 2 * 2:2]
    slack = jnp.minimum(tallies[source_of] - 1, reach - tallies[sink]) // 2
    slack = jnp.where((source_of == order[0]) | (sink == order[0]) | (tallies[sink] == 0), 0, jnp.maximum(slack, 0))
    shifted = jax.random.randint(jax.random.fold_in(own, 4), (amount // 2,), 0, 1 << 20) % (slack + 1)
    tallies = tallies.at[source_of].add(-shifted).at[sink].add(shifted)
    members = jnp.searchsorted(jnp.cumsum(tallies), jnp.arange(rows * top), side="right").astype(jnp.int32)
    grid = members.reshape(top, rows).T
    grid = grid[jax.random.permutation(jax.random.fold_in(own, 1), rows)]
    turn = jax.random.randint(jax.random.fold_in(own, 2), (rows, 1), 0, top)
    return jnp.take_along_axis(grid, (jnp.arange(top)[None, :] + turn) % top, axis=1)


def shares(count, total, limit, lean, full):
    portions = [(1 << 20) // math.isqrt(rank ** lean) + 1 for rank in range(1, count + 1)]
    largest = limit if full else min(limit, max(-(-total // count), total * portions[0] // sum(portions)))
    least = 1 if total - largest >= count - 1 else 0
    given, surplus = [largest] + [least] * (count - 1), total - largest - least * (count - 1)
    while surplus > 0:
        free = [i for i in range(1, count) if given[i] < largest] or [i for i in range(1, count) if given[i] < limit]
        pool, remaining = sum([portions[i] for i in free]), surplus
        for i in free:
            more = min(limit - given[i], max(1, remaining * portions[i] // pool), surplus)
            given[i] = given[i] + more
            surplus = surplus - more
    return np.array(given)


def bell_draw(stream_key, extent, scale, reach, cuts=(), held_as=jnp.bfloat16):
    values = scale * jax.random.normal(stream_key, extent, jnp.float32)
    if cuts:
        values = values * levels(stream_key, extent, cuts, -0.22, 0.18)
    return jnp.clip(values, -reach, reach).astype(held_as)


def setup_inputs(seed: int = 0) -> dict:
    key_of = jax.random.split(jax.random.key(seed), 9)
    act_in = draw_act_in(jax.random.fold_in(key_of[8], 71), 0)
    next_in = draw_next_in(jax.random.fold_in(key_of[8], 71), 0)
    routes_keys = jax.random.split(jax.random.fold_in(key_of[2], 1), TICKS * SECTIONS * TOKENS // TOK_DEV)
    routes_turns = jax.random.permutation(jax.random.fold_in(key_of[2], 3), TICKS * SECTIONS * TOKENS // TOK_DEV)
    routes = jax.vmap(lambda own, number: routed_block(jax.random.fold_in(key_of[2], 2), own, number, TOK_DEV, EXPERTS, TOPK, CAP, 2))(routes_keys, routes_turns).reshape((TICKS, SECTIONS, TOKENS, TOPK))
    route_w = jnp.clip(0.2 + 0.8 * jax.random.uniform(key_of[3], (TICKS, SECTIONS, TOKENS, TOPK), jnp.float32) ** levels(key_of[3], (TICKS, SECTIONS, TOKENS, TOPK), ((1, 4), (2, 8)), -0.2, 0.2), 0.2, 1.0)
    hist = jnp.clip(2.0 + 6.0 * jax.random.uniform(key_of[4], (SECTIONS,), jnp.float32) ** levels(key_of[4], (SECTIONS,), ((0, 4),), -0.2, 0.2), 2.0, 8.0)
    gate_w = bell_draw(key_of[5], (SECTIONS, EXPERTS, D, FFW), D ** -0.5, 0.0625, ((0, 4), (1, 8), (2, 8)))
    up_w = bell_draw(key_of[6], (SECTIONS, EXPERTS, D, FFW), D ** -0.5, 0.0625, ((0, 4), (1, 8), (2, 8)))
    down_w = bell_draw(key_of[7], (SECTIONS, EXPERTS, FFW, D), (4 * FFW) ** -0.5, 0.09375, ((0, 4), (1, 8), (3, 8)))
    return dict(act_in=act_in, next_in=next_in, routes=routes, route_w=route_w, hist=hist, gate_w=gate_w, up_w=up_w, down_w=down_w)


FP8_LIMIT = 448.0


def expert_rows(token_rows, gate_mat, up_mat, down_mat, dequant):
    gate_val = jnp.dot(token_rows, gate_mat, preferred_element_type=jnp.float32) * dequant
    up_val = jnp.dot(token_rows, up_mat, preferred_element_type=jnp.float32) * dequant
    hidden = (jax.nn.silu(gate_val) * up_val).astype(jnp.bfloat16)
    return jnp.dot(hidden, down_mat, preferred_element_type=jnp.float32).astype(jnp.bfloat16)


def moe_layer(stream, quant_scale, expert_of, weight_of, gate_all, up_all, down_all):
    quantized = jnp.clip(stream.astype(jnp.float32) * (FP8_LIMIT / quant_scale), -FP8_LIMIT, FP8_LIMIT).astype(jnp.bfloat16)
    dequant = quant_scale / FP8_LIMIT
    pair_count = TOKENS * TOPK
    flat_expert = expert_of.reshape(pair_count).astype(jnp.int32)
    flat_weight = weight_of.reshape(pair_count)
    slot_total = N_NODE * CAP
    positions = jnp.arange(pair_count, dtype=jnp.int32)

    def per_expert(expert_id):
        sort_keys = jnp.where(flat_expert == expert_id, positions, pair_count)
        chosen = jnp.argsort(sort_keys, stable=True)[:slot_total].astype(jnp.int32)
        is_valid = (flat_expert[chosen] == expert_id).astype(jnp.float32)
        token_ids = chosen // TOPK
        token_rows = quantized[token_ids]
        outputs = expert_rows(token_rows, gate_all[expert_id], up_all[expert_id], down_all[expert_id], dequant)
        return token_ids, outputs.astype(jnp.float32) * (flat_weight[chosen] * is_valid)[:, None]

    token_ids, contrib = lax.map(per_expert, jnp.arange(EXPERTS, dtype=jnp.int32))
    branch = jnp.zeros((TOKENS, D), jnp.float32).at[token_ids.reshape(-1)].add(contrib.reshape(-1, D))
    return (stream.astype(jnp.float32) + branch).astype(jnp.bfloat16)


def reference(act_in, next_in, routes, route_w, hist, gate_w, up_w, down_w):
    first_peaks = []
    first_tick = []
    for section_id in range(SECTIONS):
        stream = act_in[section_id]
        first_peaks.append(jnp.max(jnp.abs(stream.astype(jnp.float32))))
        first_tick.append(moe_layer(stream, hist[section_id], routes[0, section_id], route_w[0, section_id], gate_w[section_id], up_w[section_id], down_w[section_id]))
    second_peaks = []
    second_tick = []
    for section_id in range(SECTIONS):
        stream = next_in if section_id == 0 else first_tick[section_id - 1]
        second_peaks.append(jnp.max(jnp.abs(stream.astype(jnp.float32))))
        second_tick.append(moe_layer(stream, first_peaks[section_id], routes[1, section_id], route_w[1, section_id], gate_w[section_id], up_w[section_id], down_w[section_id]))
    act_out = jnp.stack([jnp.stack(first_tick), jnp.stack(second_tick)])
    peak_out = jnp.stack([jnp.stack(first_peaks), jnp.stack(second_peaks)], axis=1)
    return act_out, peak_out
```

```python
import functools
import jax
import jax.numpy as jnp
from jax import lax
from jax.experimental import pallas as pl
from jax.experimental.pallas import tpu as pltpu
from jax.sharding import Mesh
from jax.sharding import PartitionSpec as P


TORUS = ("tx", "tc")
NODE_TORUS = ("node", "tx", "tc")
FP8_LIMIT = 448.0
CHUNKS = ((0, 4, 3, 5), (1, 7, 2, 6))
BF16 = jnp.bfloat16
F32 = jnp.float32

VMEM = pl.BlockSpec(memory_space=pltpu.VMEM)
SMEM = pl.BlockSpec(memory_space=pltpu.SMEM)


def rotated(value, axis, shift):
    count = lax.axis_size(axis)
    if shift % count == 0:
        return value
    return lax.ppermute(value, axis, [(i, (i + shift) % count) for i in range(count)])


def call(kernel, outs, ins, flops, name):
    size = sum(a.size * a.dtype.itemsize for a in (*outs, *ins))
    return pl.pallas_call(
        kernel,
        out_shape=outs,
        in_specs=[SMEM if a.shape == (1, 1) else VMEM for a in ins],
        out_specs=[VMEM for _ in outs],
        cost_estimate=pl.CostEstimate(flops=flops, bytes_accessed=size, transcendentals=0),
        name=name,
    )(*ins)


def shape(dims, dtype):
    return jax.ShapeDtypeStruct(dims, dtype)


def stream_value(stream_refs):
    if len(stream_refs) == 1:
        return stream_refs[0][...].astype(F32)
    fresh, passed = stream_refs
    keep = lax.axis_index("section") == 0
    return jnp.where(keep, fresh[...].astype(F32), passed[...].astype(F32))


def dispatch_kernel(n_stream, n_node, cap, *refs):
    scale_ref, route_ref, *rest = refs
    streams, outs = rest[:n_stream], rest[n_stream:]
    *blocks, slot_ref, peak_ref = outs
    tokens = route_ref.shape[1]
    here = lax.axis_index("node")
    relative = lax.rem(route_ref[...] - here + n_node, n_node)
    ids = lax.broadcasted_iota(jnp.int32, (n_node, tokens), 0)
    hits = jnp.concatenate(
        [(ids == relative[0:1, :]).astype(F32), (ids == relative[1:2, :]).astype(F32)], axis=0
    )
    row = lax.broadcasted_iota(jnp.int32, (tokens, tokens), 0)
    column = lax.broadcasted_iota(jnp.int32, (tokens, tokens), 1)
    before = (row < column).astype(F32).astype(BF16)
    rank = jnp.dot(hits.astype(BF16), before, preferred_element_type=F32)
    first_total = jnp.sum(hits[:n_node], axis=1, keepdims=True)
    rank = rank + jnp.concatenate([jnp.zeros_like(first_total), first_total], axis=0)
    slot = jnp.where(hits > 0.5, rank, -1.0).astype(jnp.int32)
    slot_ref[...] = slot
    value = stream_value(streams)
    peak_ref[...] = jnp.full(peak_ref.shape, jnp.max(jnp.abs(value)), F32)
    factor = FP8_LIMIT / jnp.full((1, 128), scale_ref[0, 0], F32)
    quantized = jnp.clip(value * factor[:, 0:1], -FP8_LIMIT, FP8_LIMIT).astype(BF16)
    place = lax.broadcasted_iota(jnp.int32, (cap, tokens), 0)
    for k, block in enumerate(blocks):
        chosen = (place == slot[k : k + 1]) | (place == slot[n_node + k : n_node + k + 1])
        block[...] = jnp.dot(
            chosen.astype(F32).astype(BF16), quantized, preferred_element_type=F32
        ).astype(BF16)


def project_kernel(other, *refs):
    *blocks, gate_ref, up_ref, out_ref = refs
    core = lax.axis_index("tc")
    core = 1 - core if other else core
    n_x = lax.axis_size("tx")
    units = gate_ref.shape[1] // (2 * n_x)
    rows = jnp.concatenate([b[...] for b in blocks], axis=0)
    for j in range(n_x):
        at = pl.multiple_of((core * n_x + j) * units, units)
        weights = jnp.concatenate([gate_ref[:, pl.ds(at, units)], up_ref[:, pl.ds(at, units)]], axis=1)
        out_ref[:, 2 * units * j : 2 * units * (j + 1)] = jnp.dot(
            rows, weights, preferred_element_type=F32
        ).astype(out_ref.dtype)


def core_sum_kernel(own_ref, came_ref, *outs):
    n_x = lax.axis_size("tx")
    width = outs[0].shape[1]
    here = lax.axis_index("tx")
    for j, out in enumerate(outs):
        at = pl.multiple_of(lax.rem(here + j, n_x) * width, width)
        total = own_ref[:, pl.ds(at, width)] + came_ref[:, pl.ds(at, width)].astype(F32)
        out[...] = total.astype(out.dtype)


def hidden_kernel(scale_ref, own_ref, *refs):
    *came, out_ref = refs
    units = out_ref.shape[1]
    total = own_ref[...]
    for c in came:
        total = total + c[...].astype(F32)
    dequant = jnp.full((1, 128), scale_ref[0, 0], F32) / FP8_LIMIT
    total = total * dequant[:, 0:1]
    gate, up = total[:, :units], total[:, units:]
    out_ref[...] = (gate / (1.0 + jnp.exp(-gate)) * up).astype(BF16)


def join_kernel(*refs):
    *pieces, out_ref = refs
    n_x = len(pieces)
    units = pieces[0].shape[1]
    here = lax.axis_index("tx")
    for j, piece in enumerate(pieces):
        at = pl.multiple_of(lax.rem(here - j + n_x, n_x) * units, units)
        out_ref[:, pl.ds(at, units)] = piece[...]


def down_kernel(cap, own_ref, came_ref, down_ref, *outs):
    core = lax.axis_index("tc")
    half = own_ref.shape[1]
    mine = down_ref[pl.ds(pl.multiple_of(core * half, half), half), :]
    theirs = down_ref[pl.ds(pl.multiple_of((1 - core) * half, half), half), :]
    total = jnp.dot(own_ref[...], mine, preferred_element_type=F32) + jnp.dot(
        came_ref[...], theirs, preferred_element_type=F32
    )
    for i, out in enumerate(outs):
        out[...] = total[i * cap : (i + 1) * cap].astype(BF16)


def combine_kernel(n_base, chunk, n_node, slot_ref, weight_ref, *refs):
    base, rest = refs[:n_base], refs[n_base:]
    *results, out_ref = rest
    cap = results[0].shape[0]
    tokens = slot_ref.shape[1]
    slot = slot_ref[...]
    weight = weight_ref[...]
    place = lax.broadcasted_iota(jnp.int32, (cap, tokens), 0)
    parts = []
    for k in chunk:
        parts.append(
            jnp.where(place == slot[k : k + 1], weight[0:1], 0.0)
            + jnp.where(place == slot[n_node + k : n_node + k + 1], weight[1:2], 0.0)
        )
    mix = jnp.concatenate(parts, axis=0)
    high = mix.astype(BF16)
    low = (mix - high.astype(F32)).astype(BF16)
    rows = jnp.concatenate([r[...] for r in results], axis=0)
    dims = (((0,), (0,)), ((), ()))
    branch = lax.dot_general(high, rows, dims, preferred_element_type=F32) + lax.dot_general(
        low, rows, dims, preferred_element_type=F32
    )
    out_ref[...] = (stream_value(base) + branch).astype(out_ref.dtype)


def peak_over_group(x):
    count = lax.axis_size(NODE_TORUS)
    everything = lax.all_to_all(jnp.broadcast_to(x[None], (count, *x.shape)), NODE_TORUS, 0, 0, tiled=True)
    return jnp.max(everything, axis=0)


def shards(act_in, next_in, routes, route_w, hist, gate_w, up_w, down_w):
    tokens, width = act_in.shape[1:]
    n_node = lax.axis_size("node")
    n_x = lax.axis_size("tx")
    cap = 5 * tokens * routes.shape[3] // (4 * n_node)
    gate_mat, up_mat, down_mat = gate_w[0, 0], up_w[0, 0], down_w[0, 0]
    ffw = gate_mat.shape[1]
    units = ffw // (2 * n_x)
    streams = (act_in[0],)
    scale = hist.reshape(1, 1)
    outputs, peaks = [], []
    for tick in range(routes.shape[0]):
        experts = routes[tick, 0].T
        weights = route_w[tick, 0].T
        with jax.named_scope(f"t{tick}_dispatch"):
            *sent, slots, peak = call(
                functools.partial(dispatch_kernel, len(streams), n_node, cap),
                [shape((cap, width), BF16)] * n_node
                + [shape((2 * n_node, tokens), jnp.int32), shape((8, 128), F32)],
                [scale, experts, *streams],
                2 * n_node * cap * tokens * width,
                f"dispatch{tick}",
            )
        with jax.named_scope(f"t{tick}_peak"):
            group_peak = peak_over_group(peak[0, 0])
        arrived = {}
        for chunk in CHUNKS:
            for k in chunk:
                with jax.named_scope(f"t{tick}_send{k}"):
                    arrived[k] = rotated(sent[k], "node", k)
        total = streams
        for c, chunk in enumerate(CHUNKS):
            rows = cap * len(chunk)
            blocks = [arrived[k] for k in chunk]
            flops = 2 * rows * width * ffw
            with jax.named_scope(f"t{tick}_c{c}_project"):
                (away,) = call(
                    functools.partial(project_kernel, True), [shape((rows, ffw), BF16)],
                    [*blocks, gate_mat, up_mat], flops, f"project_other{tick}{c}",
                )
                came = rotated(away, "tc", 1)
                (own,) = call(
                    functools.partial(project_kernel, False), [shape((rows, ffw), F32)],
                    [*blocks, gate_mat, up_mat], flops, f"project_own{tick}{c}",
                )
                kept, *parts = call(
                    core_sum_kernel,
                    [shape((rows, 2 * units), F32)] + [shape((rows, 2 * units), BF16)] * (n_x - 1),
                    [own, came], rows * ffw, f"core_sum{tick}{c}",
                )
            with jax.named_scope(f"t{tick}_c{c}_sum"):
                partials = {j: rotated(parts[j - 1], "tx", j) for j in (2, 1, 3)}
            with jax.named_scope(f"t{tick}_c{c}_hidden"):
                (hidden,) = call(
                    hidden_kernel, [shape((rows, units), BF16)],
                    [scale, kept, partials[1], partials[2], partials[3]],
                    rows * units * 20, f"hidden{tick}{c}",
                )
            with jax.named_scope(f"t{tick}_c{c}_gather"):
                pieces = {j: rotated(hidden, "tx", j) for j in (2, 1, 3)}
                (joined,) = call(
                    join_kernel, [shape((rows, n_x * units), BF16)],
                    [hidden, pieces[1], pieces[2], pieces[3]], rows * units, f"join{tick}{c}",
                )
                other = rotated(joined, "tc", 1)
            with jax.named_scope(f"t{tick}_c{c}_down"):
                results = call(
                    functools.partial(down_kernel, cap), [shape((cap, width), BF16)] * len(chunk),
                    [joined, other, down_mat], 2 * rows * ffw * width, f"down{tick}{c}",
                )
            returned = []
            for k, result in zip(chunk, results):
                with jax.named_scope(f"t{tick}_back{k}"):
                    returned.append(rotated(result, "node", -k))
            last = c == len(CHUNKS) - 1
            with jax.named_scope(f"t{tick}_c{c}_combine"):
                total = tuple(call(
                    functools.partial(combine_kernel, len(total), chunk, n_node),
                    [shape((tokens, width), BF16 if last else F32)],
                    [slots, weights, *total, *returned],
                    4 * rows * tokens * width, f"combine{tick}{c}",
                ))
        outputs.append(total[0])
        peaks.append(group_peak)
        scale = group_peak.reshape(1, 1)
        if tick + 1 < routes.shape[0]:
            with jax.named_scope("relay"):
                sections = lax.axis_size("section")
                passed = lax.ppermute(total[0], "section", [(s, s + 1) for s in range(sections - 1)])
            streams = (next_in, passed)
    return jnp.stack(outputs)[:, None], jnp.stack(peaks)[None, :]


def solution(mesh):
    finer = Mesh(
        mesh.devices.reshape(mesh.shape["section"], mesh.shape["node"], 4, 2),
        ("section", "node", "tx", "tc"),
    )
    return jax.shard_map(
        shards,
        mesh=finer,
        in_specs=(
            P("section", "node", TORUS),
            P("node", TORUS),
            P(None, "section", "node", None),
            P(None, "section", "node", None),
            P("section"),
            P("section", "node", TORUS, None),
            P("section", "node", TORUS, None),
            P("section", "node", None, TORUS),
        ),
        out_specs=(P(None, "section", "node", TORUS), P("section", None)),
        check_vma=False,
    )
```

```python
import functools
import jax
import jax.numpy as jnp
from jax import lax
from jax.experimental import pallas as pl
from jax.experimental.pallas import tpu as pltpu
from jax.sharding import Mesh
from jax.sharding import PartitionSpec as P


TORUS = ("tx", "tc")
FP8_LIMIT = 448.0
CHUNKS = ((0, 4, 3, 5), (2, 6, 1, 7))
NODE_PEAK_ROWS = 8
PEAK_ROWS = 16
LIMIT = 14 * 1024 * 1024
BF16 = jnp.bfloat16
F32 = jnp.float32

VMEM = pl.BlockSpec(memory_space=pltpu.VMEM)
SMEM = pl.BlockSpec(memory_space=pltpu.SMEM)


def rotated(value, axis, shift):
    count = lax.axis_size(axis)
    if shift % count == 0:
        return value
    return lax.ppermute(value, axis, [(i, (i + shift) % count) for i in range(count)])


def call(kernel, outs, ins, flops, scratch=()):
    size = sum(a.size * a.dtype.itemsize for a in (*outs, *ins))
    return pl.pallas_call(
        kernel,
        out_shape=outs,
        in_specs=[SMEM if a.shape == (1, 1) else VMEM for a in ins],
        out_specs=[VMEM for _ in outs],
        scratch_shapes=list(scratch),
        compiler_params=pltpu.CompilerParams(vmem_limit_bytes=LIMIT),
        cost_estimate=pl.CostEstimate(flops=flops, bytes_accessed=size, transcendentals=0),
    )(*ins)


def shape(dims, dtype):
    return jax.ShapeDtypeStruct(dims, dtype)


def over_columns(width, body, tile=512):
    for at in range(0, width, tile):
        body(at, min(tile, width - at))


def stream_value(stream_refs, at, size):
    values = [ref[:, pl.ds(at, size)].astype(F32) for ref in stream_refs]
    if len(values) == 1:
        return values[0]
    return jnp.where(lax.axis_index("section") == 0, *values)


def scale_row(scale_refs):
    if scale_refs[0].shape == (1, 1):
        return jnp.full((1, 1), scale_refs[0][0, 0], F32)
    return scale_refs[0][0:1, 0:1]


def dispatch_kernel(tick, n_scale, n_stream, n_node, cap, *refs):
    scales, route_ref, streams = refs[:n_scale], refs[n_scale], refs[n_scale + 1 : n_scale + 1 + n_stream]
    *blocks, slot_ref, chosen_ref, quantized_ref = refs[n_scale + 1 + n_stream :]
    tokens = route_ref.shape[2]
    here = lax.axis_index("node")
    relative = lax.rem(route_ref[tick] - here + n_node, n_node)
    ids = lax.broadcasted_iota(jnp.int32, (n_node, tokens), 0)
    hits = jnp.concatenate(
        [(ids == relative[0:1, :]).astype(F32), (ids == relative[1:2, :]).astype(F32)], axis=0
    )
    row = lax.broadcasted_iota(jnp.int32, (tokens, tokens), 0)
    column = lax.broadcasted_iota(jnp.int32, (tokens, tokens), 1)
    before = (row < column).astype(F32).astype(BF16)
    rank = jnp.dot(hits.astype(BF16), before, preferred_element_type=F32)
    first_total = jnp.sum(hits[:n_node], axis=1, keepdims=True)
    rank = rank + jnp.concatenate([jnp.zeros_like(first_total), first_total], axis=0)
    slot = jnp.where(hits > 0.5, rank, -1.0).astype(jnp.int32)
    slot_ref[...] = slot
    value = stream_value(streams, 0, streams[0].shape[1])
    peak = jnp.full((NODE_PEAK_ROWS, value.shape[1]), jnp.max(jnp.abs(value)), F32).astype(BF16)
    for block in blocks:
        block[cap:, :] = peak
    factor = FP8_LIMIT / scale_row(scales)
    quantized_ref[...] = jnp.clip(value * factor, -FP8_LIMIT, FP8_LIMIT).astype(BF16)
    place = lax.broadcasted_iota(jnp.int32, (cap, tokens), 0)
    for k in range(n_node):
        chosen = (place == slot[k : k + 1]) | (place == slot[n_node + k : n_node + k + 1])
        chosen_ref[k * cap : (k + 1) * cap, :] = chosen.astype(F32).astype(BF16)

    def body(at, size):
        rows = jnp.dot(chosen_ref[...], quantized_ref[:, pl.ds(at, size)], preferred_element_type=F32)
        for k, block in enumerate(blocks):
            block[:cap, pl.ds(at, size)] = rows[k * cap : (k + 1) * cap].astype(BF16)

    over_columns(quantized_ref.shape[1], body)


def prepare_kernel(gate_ref, up_ref, weight_ref):
    units = weight_ref.shape[1] // (4 * lax.axis_size("tx"))
    for j in range(gate_ref.shape[1] // units):
        for half, source in enumerate((gate_ref, up_ref)):
            at = (2 * j + half) * units
            weight_ref[:, at : at + units] = source[:, j * units : (j + 1) * units]


def project_kernel(other, cap, n_extra, n_blocks, *refs):
    extra, refs = refs[:n_extra], refs[n_extra:]
    blocks, (weight_ref, *outs, rows_ref) = refs[:n_blocks], refs[n_blocks:]
    out_ref = outs[0]
    core = lax.axis_index("tc")
    core = 1 - core if other else core
    half = weight_ref.shape[1] // 2
    rows = cap * n_blocks
    for i, block in enumerate(blocks):
        rows_ref[i * cap : (i + 1) * cap, :] = block[:cap, :]
    if extra:
        top = functools.reduce(jnp.maximum, [b[cap:, :128].astype(F32) for b in (*extra, *blocks)])
        outs[1][...] = top
        out_ref[rows:, :] = jnp.broadcast_to(top[0:1, 0:1], (PEAK_ROWS, out_ref.shape[1])).astype(BF16)

    def body(at, size):
        where = pl.multiple_of(core * half + at, 512)
        out_ref[:rows, pl.ds(at, size)] = jnp.dot(
            rows_ref[...], weight_ref[:, pl.ds(where, size)], preferred_element_type=F32
        ).astype(out_ref.dtype)

    over_columns(half, body)


def core_sum_kernel(n_peak, *refs):
    peaks, (own_ref, came_ref, *outs) = refs[:n_peak], refs[n_peak:]
    n_x = lax.axis_size("tx")
    width = outs[0].shape[1]
    here = lax.axis_index("tx")
    rows = own_ref.shape[0]
    for j, out in enumerate(outs):
        at = pl.multiple_of(lax.rem(here + j, n_x) * width, width)
        total = own_ref[:, pl.ds(at, width)] + came_ref[:rows, pl.ds(at, width)].astype(F32)
        out[:rows, :] = total.astype(out.dtype)
        for peak in peaks:
            top = jnp.maximum(came_ref[rows:, :width].astype(F32), peak[0:1, 0:1])
            out[rows:, :] = top.astype(out.dtype)


def hidden_kernel(n_scale, n_peak, *refs):
    scales, refs = refs[:n_scale], refs[n_scale:]
    own_ref, refs = refs[0], refs[1:]
    outs = refs[len(refs) - 1 - n_peak :]
    came = refs[: len(refs) - 1 - n_peak]
    out_ref = outs[0]
    rows, units = out_ref.shape
    total = own_ref[:rows, :]
    for c in came:
        total = total + c[:rows, :].astype(F32)
    total = total * (scale_row(scales) / FP8_LIMIT)
    gate, up = total[:, :units], total[:, units:]
    out_ref[...] = (gate / (1.0 + jnp.exp(-gate)) * up).astype(BF16)
    for peak in outs[1:]:
        top = own_ref[rows : rows + 8, :128]
        for c in came:
            top = jnp.maximum(top, c[rows:, :128].astype(F32)[:8])
        peak[...] = top


def join_kernel(*refs):
    *pieces, out_ref = refs
    n_x = len(pieces)
    units = pieces[0].shape[1]
    here = lax.axis_index("tx")
    for j, piece in enumerate(pieces):
        at = pl.multiple_of(lax.rem(here - j + n_x, n_x) * units, units)
        out_ref[:, pl.ds(at, units)] = piece[...]


def down_kernel(cap, own_ref, came_ref, down_ref, *outs):
    core = lax.axis_index("tc")
    half = own_ref.shape[1]

    def body(at, size):
        mine = down_ref[pl.ds(pl.multiple_of(core * half, half), half), pl.ds(at, size)]
        theirs = down_ref[pl.ds(pl.multiple_of((1 - core) * half, half), half), pl.ds(at, size)]
        total = jnp.dot(own_ref[...], mine, preferred_element_type=F32) + jnp.dot(
            came_ref[...], theirs, preferred_element_type=F32
        )
        for i, out in enumerate(outs):
            out[:, pl.ds(at, size)] = total[i * cap : (i + 1) * cap].astype(BF16)

    over_columns(down_ref.shape[1], body)


def combine_kernel(tick, n_base, n_done, chunk, n_node, slot_ref, weight_ref, *refs):
    base, refs = refs[:n_base], refs[n_base:]
    done, refs = refs[:n_done], refs[n_done:]
    *results, out_ref, high_ref, low_ref = refs
    cap = results[0].shape[0]
    tokens = slot_ref.shape[1]
    slot = slot_ref[...]
    weight = weight_ref[tick]
    place = lax.broadcasted_iota(jnp.int32, (cap, tokens), 0)
    for i, k in enumerate(chunk):
        mix = jnp.where(place == slot[k : k + 1], weight[0:1], 0.0) + jnp.where(
            place == slot[n_node + k : n_node + k + 1], weight[1:2], 0.0
        )
        high = mix.astype(BF16)
        high_ref[:, i * cap : (i + 1) * cap] = high.T
        low_ref[:, i * cap : (i + 1) * cap] = (mix - high.astype(F32)).astype(BF16).T

    def body(at, size):
        rows = jnp.concatenate([r[:, pl.ds(at, size)] for r in results], axis=0)
        branch = jnp.dot(high_ref[...], rows, preferred_element_type=F32) + jnp.dot(
            low_ref[...], rows, preferred_element_type=F32
        )
        total = (stream_value(base, at, size) + branch).astype(out_ref.dtype)
        if done:
            out_ref[0, :, pl.ds(at, size)] = done[0][:, pl.ds(at, size)]
            out_ref[1, :, pl.ds(at, size)] = total
        else:
            out_ref[:, pl.ds(at, size)] = total

    over_columns(results[0].shape[1], body)


def shards(act_in, next_in, routes, route_w, hist, gate_w, up_w, down_w):
    tokens, width = act_in.shape[1:]
    ticks = routes.shape[0]
    n_node = lax.axis_size("node")
    n_x = lax.axis_size("tx")
    cap = 5 * tokens * routes.shape[3] // (4 * n_node)
    gate_mat, up_mat, down_mat = gate_w[0, 0], up_w[0, 0], down_w[0, 0]
    ffw = gate_mat.shape[1]
    units = ffw // (2 * n_x)
    experts = routes[:, 0].transpose(0, 2, 1)
    weights = route_w[:, 0].transpose(0, 2, 1)
    streams = (act_in[0],)
    scales = (hist.reshape(1, 1),)
    done, peaks = [], []
    for tick in range(ticks):
        *sent, slots = call(
            functools.partial(dispatch_kernel, tick, len(scales), len(streams), n_node, cap),
            [shape((cap + NODE_PEAK_ROWS, width), BF16)] * n_node
            + [shape((2 * n_node, tokens), jnp.int32)],
            [*scales, experts, *streams],
            2 * n_node * cap * tokens * width,
            [pltpu.VMEM((n_node * cap, tokens), BF16), pltpu.VMEM((tokens, width), BF16)],
        )
        if tick == 0:
            (both_mat,) = call(prepare_kernel, [shape((width, 2 * ffw), BF16)], [gate_mat, up_mat], 0)
        arrived = {}
        for chunk in CHUNKS:
            for k in chunk:
                arrived[k] = rotated(sent[k], "node", k)
        total = streams
        for c, chunk in enumerate(CHUNKS):
            rows = cap * len(chunk)
            blocks = [arrived[k] for k in chunk]
            flops = 2 * rows * width * ffw
            last = c == len(CHUNKS) - 1
            extra = [arrived[k] for chunk in CHUNKS[:-1] for k in chunk] if last else []
            long = rows + (PEAK_ROWS if last else 0)
            scratch = [pltpu.VMEM((rows, width), BF16)]
            away, *carried = call(
                functools.partial(project_kernel, True, cap, len(extra), len(blocks)),
                [shape((long, ffw), BF16)] + [shape((8, 128), F32)] * last,
                [*extra, *blocks, both_mat], flops, scratch,
            )
            came = rotated(away, "tc", 1)
            (own,) = call(
                functools.partial(project_kernel, False, cap, 0, len(blocks)),
                [shape((rows, ffw), F32)],
                [*blocks, both_mat], flops, scratch,
            )
            kept, *parts = call(
                functools.partial(core_sum_kernel, len(carried)),
                [shape((long, 2 * units), F32)] + [shape((long, 2 * units), BF16)] * (n_x - 1),
                [*carried, own, came], rows * ffw,
            )
            partials = {j: rotated(parts[j - 1], "tx", j) for j in (1, 3, 2)}
            hidden, *torus_peak = call(
                functools.partial(hidden_kernel, len(scales), len(carried)),
                [shape((rows, units), BF16)] + [shape((8, 128), F32)] * len(carried),
                [*scales, kept, partials[1], partials[2], partials[3]],
                rows * units * 20,
            )
            pieces = {j: rotated(hidden, "tx", j) for j in (1, 3, 2)}
            (joined,) = call(
                join_kernel, [shape((rows, n_x * units), BF16)],
                [hidden, pieces[1], pieces[2], pieces[3]], rows * units,
            )
            other = rotated(joined, "tc", 1)
            results = call(
                functools.partial(down_kernel, cap), [shape((cap, width), BF16)] * len(chunk),
                [joined, other, down_mat], 2 * rows * ffw * width,
            )
            returned = [rotated(r, "node", -k) for k, r in zip(chunk, results)]
            final = last and tick == ticks - 1
            if last:
                out = shape((ticks, tokens, width) if final else (tokens, width), BF16)
            else:
                out = shape((tokens, width), F32)
            total = tuple(call(
                functools.partial(combine_kernel, tick, len(total), len(done) if final else 0, chunk, n_node),
                [out],
                [slots, weights, *total, *(done if final else []), *returned],
                4 * rows * tokens * width,
                [pltpu.VMEM((tokens, rows), BF16)] * 2,
            ))
        scales = tuple(torus_peak)
        peaks.append(torus_peak[0][0, 0])
        if tick + 1 < ticks:
            done.append(total[0])
            sections = lax.axis_size("section")
            passed = lax.ppermute(total[0], "section", [(s, s + 1) for s in range(sections - 1)])
            streams = (next_in, passed)
    return total[0][:, None], jnp.stack(peaks)[None, :]


def solution(mesh):
    finer = Mesh(
        mesh.devices.reshape(mesh.shape["section"], mesh.shape["node"], 4, 2),
        ("section", "node", "tx", "tc"),
    )

    return jax.shard_map(
        shards,
        mesh=finer,
        in_specs=(
            P("section", "node", TORUS),
            P("node", TORUS),
            P(None, "section", "node", None),
            P(None, "section", "node", None),
            P("section"),
            P("section", "node", TORUS, None),
            P("section", "node", TORUS, None),
            P("section", "node", None, TORUS),
        ),
        out_specs=(P(None, "section", "node", TORUS), P("section", None)),
        check_vma=False,
    )
```

```python
import functools
import jax
import jax.numpy as jnp
from jax import lax
from jax.experimental import pallas as pl
from jax.experimental.pallas import tpu as pltpu
from jax.sharding import Mesh
from jax.sharding import PartitionSpec as P


TORUS = ("tx", "tc")
FP8_LIMIT = 448.0
CHUNKS = ((4, 3, 5), (0, 2, 6, 1, 7))
NODE_PEAK_ROWS = 8
PEAK_ROWS = 16
LIMIT = 14 * 1024 * 1024
BF16 = jnp.bfloat16
F32 = jnp.float32

VMEM = pl.BlockSpec(memory_space=pltpu.VMEM)
SMEM = pl.BlockSpec(memory_space=pltpu.SMEM)


def rotated(value, axis, shift):
    count = lax.axis_size(axis)
    if shift % count == 0:
        return value
    return lax.ppermute(value, axis, [(i, (i + shift) % count) for i in range(count)])


def call(kernel, outs, ins, flops, scratch=()):
    size = sum(a.size * a.dtype.itemsize for a in (*outs, *ins))
    return pl.pallas_call(
        kernel,
        out_shape=outs,
        in_specs=[SMEM if a.shape == (1, 1) else VMEM for a in ins],
        out_specs=[VMEM for _ in outs],
        scratch_shapes=list(scratch),
        compiler_params=pltpu.CompilerParams(vmem_limit_bytes=LIMIT),
        cost_estimate=pl.CostEstimate(flops=flops, bytes_accessed=size, transcendentals=0),
    )(*ins)


def shape(dims, dtype):
    return jax.ShapeDtypeStruct(dims, dtype)


def over_columns(width, body, tile=512):
    for at in range(0, width, tile):
        body(at, min(tile, width - at))


def dispatch_kernel(
    n_node, cap, tick_ref, first_ref, before_ref, route_ref, route_w_ref, fresh_ref, passed_ref, *refs
):
    *blocks, slot_ref, weight_ref, scale_ref, stream_ref, chosen_ref, quantized_ref = refs
    tick = tick_ref[0, 0].astype(jnp.int32)
    scale = jnp.where(tick == 0, jnp.full((1, 1), first_ref[0, 0], F32), before_ref[0:1, 1:2])
    scale_ref[...] = jnp.broadcast_to(scale, scale_ref.shape)
    weight_ref[...] = route_w_ref[tick]
    tokens = route_ref.shape[2]
    here = lax.axis_index("node")
    relative = lax.rem(route_ref[tick] - here + n_node, n_node)
    ids = lax.broadcasted_iota(jnp.int32, (n_node, tokens), 0)
    hits = jnp.concatenate(
        [(ids == relative[0:1, :]).astype(F32), (ids == relative[1:2, :]).astype(F32)], axis=0
    )
    row = lax.broadcasted_iota(jnp.int32, (tokens, tokens), 0)
    column = lax.broadcasted_iota(jnp.int32, (tokens, tokens), 1)
    before = (row < column).astype(F32).astype(BF16)
    rank = jnp.dot(hits.astype(BF16), before, preferred_element_type=F32)
    first_total = jnp.sum(hits[:n_node], axis=1, keepdims=True)
    rank = rank + jnp.concatenate([jnp.zeros_like(first_total), first_total], axis=0)
    slot = jnp.where(hits > 0.5, rank, -1.0).astype(jnp.int32)
    slot_ref[...] = slot
    keep = (lax.axis_index("section") == 0) & (tick > 0)
    value = jnp.where(keep, fresh_ref[...].astype(F32), passed_ref[...].astype(F32))
    stream_ref[...] = value
    peak = jnp.full((NODE_PEAK_ROWS, value.shape[1]), jnp.max(jnp.abs(value)), F32).astype(BF16)
    for block in blocks:
        block[cap:, :] = peak
    factor = FP8_LIMIT / scale
    quantized_ref[...] = jnp.clip(value * factor, -FP8_LIMIT, FP8_LIMIT).astype(BF16)
    place = lax.broadcasted_iota(jnp.int32, (cap, tokens), 0)
    for k in range(n_node):
        chosen = (place == slot[k : k + 1]) | (place == slot[n_node + k : n_node + k + 1])
        chosen_ref[k * cap : (k + 1) * cap, :] = chosen.astype(F32).astype(BF16)

    def body(at, size):
        rows = jnp.dot(chosen_ref[...], quantized_ref[:, pl.ds(at, size)], preferred_element_type=F32)
        for k, block in enumerate(blocks):
            block[:cap, pl.ds(at, size)] = rows[k * cap : (k + 1) * cap].astype(BF16)

    over_columns(quantized_ref.shape[1], body)


def prepare_kernel(tick_ref, gate_ref, up_ref, down_ref, weight_ref, near_ref):
    units = weight_ref.shape[1] // (4 * lax.axis_size("tx"))
    for j in range(gate_ref.shape[1] // units):
        for half, source in enumerate((gate_ref, up_ref)):
            at = (2 * j + half) * units
            weight_ref[:, at : at + units] = source[:, j * units : (j + 1) * units]
    near_ref[...] = down_ref[...]


def project_kernel(other, cap, n_extra, n_blocks, *refs):
    extra, refs = refs[:n_extra], refs[n_extra:]
    blocks, (weight_ref, *outs, rows_ref) = refs[:n_blocks], refs[n_blocks:]
    out_ref = outs[0]
    core = lax.axis_index("tc")
    core = 1 - core if other else core
    half = weight_ref.shape[1] // 2
    rows = cap * n_blocks
    for i, block in enumerate(blocks):
        rows_ref[i * cap : (i + 1) * cap, :] = block[:cap, :]
    if extra:
        top = functools.reduce(jnp.maximum, [b[cap:, :128].astype(F32) for b in (*extra, *blocks)])
        outs[1][...] = top
        out_ref[rows:, :] = jnp.broadcast_to(top[0:1, 0:1], (PEAK_ROWS, out_ref.shape[1])).astype(BF16)

    def body(at, size):
        where = pl.multiple_of(core * half + at, 512)
        out_ref[:rows, pl.ds(at, size)] = jnp.dot(
            rows_ref[...], weight_ref[:, pl.ds(where, size)], preferred_element_type=F32
        ).astype(out_ref.dtype)

    over_columns(half, body)


def core_sum_kernel(n_peak, *refs):
    peaks, (own_ref, came_ref, *outs) = refs[:n_peak], refs[n_peak:]
    n_x = lax.axis_size("tx")
    width = outs[0].shape[1]
    here = lax.axis_index("tx")
    rows = own_ref.shape[0]
    for j, out in enumerate(outs):
        at = pl.multiple_of(lax.rem(here + j, n_x) * width, width)
        total = own_ref[:, pl.ds(at, width)] + came_ref[:rows, pl.ds(at, width)].astype(F32)
        out[:rows, :] = total.astype(out.dtype)
        for peak in peaks:
            top = jnp.maximum(came_ref[rows:, :width].astype(F32), peak[0:1, 0:1])
            out[rows:, :] = top.astype(out.dtype)


def hidden_kernel(n_peak, scale_ref, own_ref, *refs):
    outs = refs[len(refs) - 1 - n_peak :]
    came = refs[: len(refs) - 1 - n_peak]
    out_ref = outs[0]
    rows, units = out_ref.shape
    total = own_ref[:rows, :]
    for c in came:
        total = total + c[:rows, :].astype(F32)
    total = total * (scale_ref[0:1, 0:1] / FP8_LIMIT)
    gate, up = total[:, :units], total[:, units:]
    out_ref[...] = (gate / (1.0 + jnp.exp(-gate)) * up).astype(BF16)
    for peak in outs[1:]:
        top = own_ref[rows : rows + 8, :128]
        for c in came:
            top = jnp.maximum(top, c[rows:, :128].astype(F32)[:8])
        lane = lax.broadcasted_iota(jnp.int32, top.shape, 1)
        peak[...] = jnp.where(lane == 0, scale_ref[...], top)


def join_kernel(*refs):
    *pieces, out_ref = refs
    n_x = len(pieces)
    units = pieces[0].shape[1]
    here = lax.axis_index("tx")
    for j, piece in enumerate(pieces):
        at = pl.multiple_of(lax.rem(here - j + n_x, n_x) * units, units)
        out_ref[:, pl.ds(at, units)] = piece[...]


def down_kernel(cap, own_ref, came_ref, down_ref, *outs):
    core = lax.axis_index("tc")
    half = own_ref.shape[1]

    def body(at, size):
        mine = down_ref[pl.ds(pl.multiple_of(core * half, half), half), pl.ds(at, size)]
        theirs = down_ref[pl.ds(pl.multiple_of((1 - core) * half, half), half), pl.ds(at, size)]
        total = jnp.dot(own_ref[...], mine, preferred_element_type=F32) + jnp.dot(
            came_ref[...], theirs, preferred_element_type=F32
        )
        for i, out in enumerate(outs):
            out[:, pl.ds(at, size)] = total[i * cap : (i + 1) * cap].astype(BF16)

    over_columns(down_ref.shape[1], body)


def combine_kernel(chunk, n_node, slot_ref, weight_ref, base_ref, *refs):
    *results, out_ref, high_ref, low_ref = refs
    cap = results[0].shape[0]
    tokens = slot_ref.shape[1]
    slot = slot_ref[...]
    weight = weight_ref[...]
    place = lax.broadcasted_iota(jnp.int32, (cap, tokens), 0)
    for i, k in enumerate(chunk):
        mix = jnp.where(place == slot[k : k + 1], weight[0:1], 0.0) + jnp.where(
            place == slot[n_node + k : n_node + k + 1], weight[1:2], 0.0
        )
        high = mix.astype(BF16)
        high_ref[:, i * cap : (i + 1) * cap] = high.T
        low_ref[:, i * cap : (i + 1) * cap] = (mix - high.astype(F32)).astype(BF16).T

    def body(at, size):
        rows = jnp.concatenate([r[:, pl.ds(at, size)] for r in results], axis=0)
        branch = jnp.dot(high_ref[...], rows, preferred_element_type=F32) + jnp.dot(
            low_ref[...], rows, preferred_element_type=F32
        )
        out_ref[:, pl.ds(at, size)] = (base_ref[:, pl.ds(at, size)] + branch).astype(out_ref.dtype)

    over_columns(results[0].shape[1], body)


def shards(act_in, next_in, routes, route_w, hist, gate_w, up_w, down_w):
    tokens, width = act_in.shape[1:]
    ticks = routes.shape[0]
    n_node = lax.axis_size("node")
    n_x = lax.axis_size("tx")
    cap = 5 * tokens * routes.shape[3] // (4 * n_node)
    gate_mat, up_mat, down_mat = gate_w[0, 0], up_w[0, 0], down_w[0, 0]
    ffw = gate_mat.shape[1]
    units = ffw // (2 * n_x)
    experts = routes[:, 0].transpose(0, 2, 1)
    all_weights = route_w[:, 0].transpose(0, 2, 1)
    first = hist.reshape(1, 1)

    def one_tick(carry, _):
        outputs, before, peak_before, now = carry
        tick = now.reshape(1, 1)

        def relayed(value):
            sections = lax.axis_size("section")
            return lax.ppermute(value, "section", [(s, s + 1) for s in range(sections - 1)])

        passed = lax.cond(now > 0.5, relayed, lambda value: value, before)
        *sent, slots, weights, scale, stream = call(
            functools.partial(dispatch_kernel, n_node, cap),
            [shape((cap + NODE_PEAK_ROWS, width), BF16)] * n_node
            + [shape((2 * n_node, tokens), jnp.int32), shape((2, tokens), F32), shape((8, 128), F32)]
            + [shape((tokens, width), F32)],
            [tick, first, peak_before, experts, all_weights, next_in, passed],
            2 * n_node * cap * tokens * width,
            [pltpu.VMEM((n_node * cap, tokens), BF16), pltpu.VMEM((tokens, width), BF16)],
        )
        both_mat, down_near = call(
            prepare_kernel, [shape((width, 2 * ffw), BF16), shape(down_mat.shape, BF16)],
            [tick, gate_mat, up_mat, down_mat], 0,
        )
        arrived = {}
        for chunk in CHUNKS:
            for k in chunk:
                arrived[k] = rotated(sent[k], "node", k)
        total = stream
        for c, chunk in enumerate(CHUNKS):
            rows = cap * len(chunk)
            blocks = [arrived[k] for k in chunk]
            flops = 2 * rows * width * ffw
            last = c == len(CHUNKS) - 1
            extra = [arrived[k] for chunk in CHUNKS[:-1] for k in chunk] if last else []
            long = rows + (PEAK_ROWS if last else 0)
            scratch = [pltpu.VMEM((rows, width), BF16)]
            away, *carried = call(
                functools.partial(project_kernel, True, cap, len(extra), len(blocks)),
                [shape((long, ffw), BF16)] + [shape((8, 128), F32)] * last,
                [*extra, *blocks, both_mat], flops, scratch,
            )
            came = rotated(away, "tc", 1)
            (own,) = call(
                functools.partial(project_kernel, False, cap, 0, len(blocks)),
                [shape((rows, ffw), F32)],
                [*blocks, both_mat], flops, scratch,
            )
            kept, *parts = call(
                functools.partial(core_sum_kernel, len(carried)),
                [shape((long, 2 * units), F32)] + [shape((long, 2 * units), BF16)] * (n_x - 1),
                [*carried, own, came], rows * ffw,
            )
            partials = {j: rotated(parts[j - 1], "tx", j) for j in (1, 3, 2)}
            hidden, *torus_peak = call(
                functools.partial(hidden_kernel, len(carried)),
                [shape((rows, units), BF16)] + [shape((8, 128), F32)] * len(carried),
                [scale, kept, partials[1], partials[2], partials[3]],
                rows * units * 20,
            )
            pieces = {j: rotated(hidden, "tx", j) for j in (1, 3, 2)}
            (joined,) = call(
                join_kernel, [shape((rows, n_x * units), BF16)],
                [hidden, pieces[1], pieces[2], pieces[3]], rows * units,
            )
            other = rotated(joined, "tc", 1)
            results = call(
                functools.partial(down_kernel, cap), [shape((cap, width), BF16)] * len(chunk),
                [joined, other, down_near], 2 * rows * ffw * width,
            )
            returned = [rotated(r, "node", -k) for k, r in zip(chunk, results)]
            (total,) = call(
                functools.partial(combine_kernel, chunk, n_node),
                [shape((tokens, width), BF16 if last else F32)],
                [slots, weights, total, *returned],
                4 * rows * tokens * width,
                [pltpu.VMEM((tokens, rows), BF16)] * 2,
            )
        outputs = lax.dynamic_update_index_in_dim(outputs, total, now.astype(jnp.int32), 0)
        return (outputs, total, torus_peak[0], now + 1.0), None

    start = (jnp.zeros((ticks, tokens, width), BF16), act_in[0], jnp.zeros((8, 128), F32), F32(0.0))
    (outputs, _, peaks, _), _ = lax.scan(one_tick, start, None, length=ticks)
    return outputs[:, None], peaks[0:1, 0:2]


def solution(mesh):
    finer = Mesh(
        mesh.devices.reshape(mesh.shape["section"], mesh.shape["node"], 4, 2),
        ("section", "node", "tx", "tc"),
    )

    return jax.shard_map(
        shards,
        mesh=finer,
        in_specs=(
            P("section", "node", TORUS),
            P("node", TORUS),
            P(None, "section", "node", None),
            P(None, "section", "node", None),
            P("section"),
            P("section", "node", TORUS, None),
            P("section", "node", TORUS, None),
            P("section", "node", None, TORUS),
        ),
        out_specs=(P(None, "section", "node", TORUS), P("section", None)),
        check_vma=False,
    )
```
